256 devices in a mesh: row: 16 (over z, x_lo), col: 16 (over x_hi, y, core).
Axes of the slice: x: 4 (x_hi: 2, x_lo: 2; x = x_hi * 2 + x_lo), y: 4, z: 8, core: 2. Of those that a mesh axis runs over, the one named last changes fastest.
Arguments:
- tiles: bfloat16 [16, 16, 3, 256, 256], P('row', 'col'), as said below
- stack_index: int32 [16, 16, 3], P('row', 'col'), may hold values from 0 to 15, as said below
- block_mask: int32 [64, 64], replicated, may hold values from 0 to 1, as said below
Outputs:
- purified: bfloat16 [16, 16, 3, 256, 256], P('row', 'col')
The draws below stay inside these ranges and needn't reach their ends.
Inputs may be any that keep to these rules, and one draw needn't show every extreme that they name: `block_mask`: the region of one device (4 x 4 blocks) holds at most 3 occupied blocks; some region holds exactly 3 in every draw. `stack_index`: block (a, b) of a device's region is numbered a * 4 + b. A device's 3 entries are distinct and include every occupied block of its region; a slot naming an unoccupied block holds a tile that P does not use. `tiles`: A slot's tile is P's block named by stack_index when that block is occupied.
All inputs are finite; a program needn't handle non-finite values.
Results may differ from the reference program's by a relative error of at most 0.0051.
Values may be sent and summed in bfloat16 or wider, within the bound.
A program may use at most 64 MiB of HBM per device.

```python
import jax
import jax.numpy as jnp
from jax import lax

NB = 64
BS = 256
SLOTS = 3
BR = 4
BC = 4
N_ROW = 16
N_COL = 16


def to_regions(table):
    return table.reshape(N_ROW, BR, N_COL, BC).transpose(0, 2, 1, 3).reshape(N_ROW, N_COL, BR * BC)


def block_layout(key):
    cluster_key = jax.random.fold_in(key, 301)
    anchor_row_key = jax.random.fold_in(key, 302)
    anchor_col_key = jax.random.fold_in(key, 303)
    noise_key = jax.random.fold_in(key, 304)
    mixing_key = jax.random.fold_in(key, 305)
    cluster = jax.random.randint(cluster_key, (NB,), 0, max(NB // 8, 1), dtype=jnp.int32)
    row_iota = jnp.arange(NB, dtype=jnp.int32)[:, None]
    col_iota = jnp.arange(NB, dtype=jnp.int32)[None, :]
    anchor_row = jax.random.randint(anchor_row_key, (), 0, N_ROW, dtype=jnp.int32)
    anchor_col = jax.random.randint(anchor_col_key, (), 0, N_COL, dtype=jnp.int32)
    favoured = (row_iota // BR == anchor_row) & (col_iota // BC == anchor_col)
    candidate = ((cluster[:, None] == cluster[None, :]) | favoured).astype(jnp.int32)
    noise_draw = jax.random.randint(noise_key, (NB, NB), 0, 1024, dtype=jnp.int32)
    priority = candidate * 4096 + noise_draw
    local_count = BR * BC
    local_iota = jnp.arange(local_count, dtype=jnp.int32)
    region_priority = to_regions(priority) * local_count + local_iota
    _, picked = lax.top_k(region_priority, SLOTS)
    picked = picked.astype(jnp.int32)
    kept_slot = jnp.sum((picked[:, :, :, None] == local_iota[None, None, None, :]).astype(jnp.int32), axis=2)
    region_mask = to_regions(candidate) * kept_slot
    occupied = region_mask.reshape(N_ROW, N_COL, BR, BC).transpose(0, 2, 1, 3).reshape(NB, NB)
    mixing = jax.random.randint(mixing_key, (N_ROW, N_COL, SLOTS), 0, 4096, dtype=jnp.int32) * SLOTS + jnp.arange(SLOTS, dtype=jnp.int32)
    placement = jnp.argsort(mixing, axis=2)
    stack_ids = jnp.take_along_axis(picked, placement, axis=2)
    return (occupied, stack_ids)


def draw_block_mask(key, part):
    return block_layout(key)[0]


def draw_stack_index(key, part):
    return block_layout(key)[1]


def draw_tiles(key, part):
    occupied, stack_ids = block_layout(key)
    noise_key = jax.random.fold_in(key, 201)
    tile_shape = (N_ROW, N_COL, SLOTS, BS, BS)
    spread = 1.0 / BS ** 0.5
    noise_draw = spread * jax.random.normal(noise_key, tile_shape, jnp.float32)
    band_row = jnp.arange(N_ROW, dtype=jnp.int32)[:, None, None]
    band_col = jnp.arange(N_COL, dtype=jnp.int32)[None, :, None]
    on_diagonal = band_row * BR + stack_ids // BC == band_col * BC + stack_ids % BC
    identity = jnp.eye(BS, dtype=jnp.float32)
    values = noise_draw + 0.5 * on_diagonal.astype(jnp.float32)[:, :, :, None, None] * identity
    return values.astype(jnp.bfloat16)


def setup_inputs(seed: int = 0) -> dict:
    key_of = jax.random.split(jax.random.key(seed), 4)
    return {
        "tiles": draw_tiles(jax.random.fold_in(key_of[3], 71), 0),
        "stack_index": draw_stack_index(jax.random.fold_in(key_of[3], 71), 0),
        "block_mask": draw_block_mask(jax.random.fold_in(key_of[3], 71), 0),
    }


def reference(tiles, stack_index, block_mask):
    total_slots = N_ROW * N_COL * SLOTS
    flat_tiles = tiles.reshape(total_slots, BS, BS)
    places = jnp.arange(total_slots, dtype=jnp.int32)
    device_id = places // SLOTS
    device_row = device_id // N_COL
    device_col = device_id % N_COL
    flat_ids = stack_index.reshape(total_slots).astype(jnp.int32)
    global_row = (device_row * BR + flat_ids // BC).astype(jnp.int32)
    global_col = (device_col * BC + flat_ids % BC).astype(jnp.int32)
    valid = block_mask[global_row, global_col] > 0
    slot_of = jnp.zeros((NB, NB), jnp.int32).at[global_row, global_col].set(places)

    def product(left_flat, right_flat):
        def per_slot(columns):
            block_row, block_col, live = columns

            def compute(unused):
                def inner(inner_block, total):
                    weight = block_mask[block_row, inner_block] * block_mask[inner_block, block_col]

                    def add_term(running):
                        left_tile = left_flat[slot_of[block_row, inner_block]]
                        right_tile = right_flat[slot_of[inner_block, block_col]]
                        return running + jnp.dot(left_tile, right_tile, preferred_element_type=jnp.float32)

                    def keep_term(running):
                        return running

                    return lax.cond(weight > 0, add_term, keep_term, total)

                return lax.fori_loop(0, NB, inner, jnp.zeros((BS, BS), jnp.float32))

            def skipped(unused):
                return jnp.zeros((BS, BS), jnp.float32)

            return lax.cond(live, compute, skipped, 0)

        return lax.map(per_slot, (global_row, global_col, valid))

    square = product(flat_tiles, flat_tiles).astype(jnp.bfloat16)
    cube_sum = product(square, flat_tiles)
    valid_float = valid.astype(jnp.float32)
    purified = (3.0 * square.astype(jnp.float32) - 2.0 * cube_sum) * valid_float[:, None, None]
    return purified.astype(jnp.bfloat16).reshape(N_ROW, N_COL, SLOTS, BS, BS)
```

```python
import functools

import jax
import jax.numpy as jnp
from jax import lax
from jax.experimental import pallas as pl
from jax.experimental.pallas import tpu as pltpu
from jax.sharding import PartitionSpec as P

MESH = pl.DeviceIdType.MESH
BS = 256
HALF = BS // 2
SENDS = 200
ZERO = 48


def device(z, xlo, xhi, y, core):
    return (z * 2 + xlo, (xhi * 4 + y) * 2 + core)


def kernel(
    tiles, stack, mask, out,
    colbuf, rowbuf, sqbuf, stage, acc, near_table, far_table,
    send_sem, col_sem, row_sem, sq_sem,
):
    r = lax.axis_index("row")
    c = lax.axis_index("col")
    z, xlo = r // 2, r % 2
    xhi, y, core = c // 8, (c // 2) % 4, c % 2
    sign = 1 - 2 * core
    xlo2, xhi2, core2 = 1 - xlo, 1 - xhi, 1 - core

    def zat(steps):
        return (z + sign * steps + 8) % 8

    def yat(steps):
        return (y + steps + 4) % 4

    to_za = device(zat(1), xlo, xhi, y, core)
    to_zb = device(zat(-1), xlo, xhi, y, core)
    to_yc = device(z, xlo, xhi, yat(1), core)
    to_yd = device(z, xlo, xhi, yat(-1), core)
    to_xlo = device(z, xlo2, xhi, y, core)
    to_xhi = device(z, xlo, xhi2, y, core)
    to_core = device(z, xlo, xhi, y, core2)
    peers = (to_za, to_zb, to_yc, to_yd, to_xlo, to_xhi, to_core)

    barrier = pltpu.get_barrier_semaphore()
    for peer in peers:
        pl.semaphore_signal(barrier, inc=1, device_id=peer, device_id_type=MESH)

    ids = [stack[0, 0, s] for s in range(3)]
    live = [mask[4 * r + ids[s] // 4, 4 * c + ids[s] % 4] > 0 for s in range(3)]
    rank = []
    for s in range(3):
        below = jnp.int32(0)
        for t in range(3):
            if t != s:
                below = below + jnp.where(live[t] & (ids[t] < ids[s]), 1, 0)
        rank.append(jnp.where(live[s], below, 3))
    own_ids = []
    for q in range(3):
        place = jnp.int32(0)
        own_id = jnp.int32(-1)
        for s in range(3):
            place = jnp.where(rank[s] == q, s, place)
            own_id = jnp.where(rank[s] == q, ids[s], own_id)
        own_ids.append(own_id)
        tile = tiles[place]
        colbuf[3 * r + q] = tile
        rowbuf[3 * c + q] = tile
    zero = jnp.zeros((BS, BS), jnp.bfloat16)
    stage[3] = zero
    colbuf[ZERO] = zero
    acc[...] = jnp.zeros_like(acc)

    pl.semaphore_wait(barrier, len(peers))

    started = []

    def piece(buf, place, part):
        if part is None:
            return buf.at[place]
        return buf.at[place, pl.ds(part * HALF, HALF)]

    def remote(buf, sems, region, unit, target):
        slot, part = {0: (0, None), 1: (1, None), 2: (2, None), 3: (2, 0), 4: (2, 1)}[unit]
        ref = piece(buf, 3 * region + slot, part)
        sem = sems.at[4 * region + {0: 0, 1: 1, 2: 2, 3: 2, 4: 3}[unit]]
        return pltpu.make_async_remote_copy(
            src_ref=ref, dst_ref=ref, send_sem=send_sem.at[len(started)], recv_sem=sem,
            device_id=target, device_id_type=MESH,
        )

    def send(buf, sems, region, unit, *targets):
        for target in targets:
            copy = remote(buf, sems, region, unit, target)
            copy.start()
            started.append(copy)

    def landed(buf, sems, region, *units):
        for unit in units:
            remote(buf, sems, region, unit, to_core).wait_recv()

    col = (colbuf, col_sem)

    def own_row(steps):
        return 2 * zat(steps) + xlo

    def par_row(steps):
        return 2 * zat(steps) + xlo2

    def cat(by, steps, own_core=True, own_xhi=True):
        return ((xhi if own_xhi else xhi2) * 4 + yat(steps)) * 2 + (core if own_core else core2)

    class Row:
        def __init__(self, buf, sems, x_first, y_first):
            self.b = (buf, sems)
            self.xf, self.yf = x_first, y_first

        def begin(self):
            me = cat("y", 0)
            for s in self.xf:
                send(*self.b, me, s, to_xhi)
            for s in self.yf + self.xf:
                send(*self.b, me, s, to_yc, to_yd)
            for s in self.yf:
                send(*self.b, me, s, to_xhi)
            for s in range(3):
                send(*self.b, me, s, to_core)

        def x_hop(self):
            par = cat("y", 0, own_xhi=False)
            for s in self.xf:
                landed(*self.b, par, s)
                send(*self.b, par, s, to_yc, to_yd, to_core)

        def y_near_first(self):
            for s in self.yf:
                for way, target, unit in ((-1, to_yc, 3), (1, to_yd, 4)):
                    region = cat("y", way)
                    landed(*self.b, region, s)
                    send(*self.b, region, unit, target)
                    send(*self.b, region, s, to_xhi, to_core)

        def y_near_own(self):
            for s in self.xf:
                landed(*self.b, cat("y", -1), s)
                send(*self.b, cat("y", -1), s, to_yc, to_core)
                landed(*self.b, cat("y", 1), s)
                send(*self.b, cat("y", 1), s, to_core)

        def y_near_par(self):
            for s in self.xf:
                landed(*self.b, cat("y", 1, own_xhi=False), s)
                send(*self.b, cat("y", 1, own_xhi=False), s, to_yd, to_core)
                landed(*self.b, cat("y", -1, own_xhi=False), s)
                send(*self.b, cat("y", -1, own_xhi=False), s, to_core)

        def x_late(self, *steps):
            for step in steps:
                for s in self.yf:
                    region = cat("y", step, own_xhi=False)
                    landed(*self.b, region, s)
                    send(*self.b, region, s, to_core)

        def y_far_first(self):
            for s in self.yf:
                region = cat("y", 2)
                for unit in (3, 4):
                    landed(*self.b, region, unit)
                    send(*self.b, region, unit, to_xhi)
                send(*self.b, region, s, to_core)

        def y_far(self):
            for s in self.xf:
                landed(*self.b, cat("y", 2), s)
                send(*self.b, cat("y", 2), s, to_core)
                landed(*self.b, cat("y", 2, own_xhi=False), s)
                send(*self.b, cat("y", 2, own_xhi=False), s, to_core)

        def x_last(self):
            for s in self.yf:
                region = cat("y", 2, own_xhi=False)
                landed(*self.b, region, 3, 4)
                send(*self.b, region, s, to_core)

        def sibling(self, steps, own_xhi=True):
            landed(*self.b, cat("y", steps, own_core=False, own_xhi=own_xhi), 0, 1, 2)

    def z_near(steps, *units, last=False):
        for unit in units:
            own = unit in (0, 1, 2)
            slot = unit if own else unit - 3
            for way in (1, -1):
                region = own_row(-way * steps) if own else par_row(-way * steps)
                target = to_za if way == 1 else to_zb
                landed(*col, region, slot)
                if not last:
                    send(*col, region, slot, target)
                elif slot == 2:
                    send(*col, region, 3 if way == 1 else 4, target)
                elif own == (way == 1):
                    send(*col, region, slot, target)
                if slot == 2:
                    send(*col, region, 2, to_xlo)

    row = Row(rowbuf, row_sem, [0, 1, 2], [])
    sq = Row(sqbuf, sq_sem, [0, 1], [2])

    send(*col, r, 0, to_xlo)
    send(*col, r, 1, to_xlo)
    for s in (2, 0, 1):
        send(*col, r, s, to_za, to_zb)
    send(*col, r, 2, to_xlo)
    row.begin()

    def table(p, carry):
        left = [jnp.int32(-1)] * 3
        count = jnp.int32(0)
        for b in range(16):
            here = mask[4 * r + b // 4, 4 * p + b % 4] > 0
            for l in range(3):
                left[l] = jnp.where(here & (count == l), b, left[l])
            count = count + jnp.where(here, 1, 0)
        word = jnp.int32(0)
        count = jnp.int32(0)
        places = []
        for b in range(16):
            here = mask[4 * p + b // 4, 4 * c + b % 4] > 0
            places.append(jnp.where(here, count, 3))
            count = count + jnp.where(here, 1, 0)
        for q in range(3):
            own = own_ids[q]
            column = [jnp.int32(3)] * 4
            for kk in range(4):
                for b in range(4):
                    column[kk] = jnp.where(own % 4 == b, places[4 * kk + b], column[kk])
            for l in range(3):
                found = jnp.int32(3)
                for kk in range(4):
                    found = jnp.where(left[l] % 4 == kk, column[kk], found)
                good = (own >= 0) & (left[l] >= 0) & (left[l] // 4 == own // 4)
                found = jnp.where(good, found, 3)
                near_table[p, 3 * q + l] = found
                far_table[p, 3 * q + l] = jnp.where(found < 3, 3 * p + found, ZERO)
        return carry

    lax.fori_loop(0, 16, table, 0)

    def near_step(p):
        for s in range(3):
            stage[s] = colbuf[3 * p + s]
        for q in range(3):
            total = acc[q]
            for l in range(3):
                total = total + jnp.dot(
                    rowbuf[3 * p + l], stage[near_table[p, 3 * q + l]],
                    preferred_element_type=jnp.float32,
                )
            acc[q] = total

    def far_step(p):
        for q in range(3):
            total = acc[q]
            for l in range(3):
                total = total + jnp.dot(
                    sqbuf[3 * p + l], colbuf[far_table[p, 3 * q + l]],
                    preferred_element_type=jnp.float32,
                )
            acc[q] = total

    def each(count, where, step):
        def body(i, carry):
            step(where(i))
            return carry

        lax.fori_loop(0, count, body, 0)

    def ring_region(steps):
        return lambda i: 2 * zat((1 - 2 * (i // 2)) * steps) + i % 2

    z_near(1, 2)
    landed(*col, par_row(0), 0)
    send(*col, par_row(0), 0, to_za, to_zb)
    landed(*col, par_row(0), 1)
    send(*col, par_row(0), 1, to_za, to_zb)
    z_near(1, 0, 1)
    row.y_near_own()
    row.x_hop()
    z_near(1, 3, 4)
    row.y_near_par()
    z_near(2, 2, 0, 1)
    row.y_far()
    z_near(2, 3, 4)
    for steps in (0, 1, -1, 2):
        row.sibling(steps)
        row.sibling(steps, own_xhi=False)
    landed(*col, par_row(0), 2)
    each(2, lambda i: 2 * z + i, near_step)
    z_near(3, 2, last=True)
    for way in (1, -1):
        landed(*col, par_row(way), 2)
    each(4, ring_region(1), near_step)
    z_near(3, 0, last=True)
    for way in (2, -2):
        landed(*col, par_row(way), 2)
    each(4, ring_region(2), near_step)
    z_near(3, 1, 3, 4, last=True)
    landed(*col, own_row(4), 3)
    send(*col, own_row(4), 3, to_xlo)
    landed(*col, own_row(4), 4)
    send(*col, own_row(4), 4, to_xlo)
    for way in (3, -3):
        landed(*col, par_row(way), 2)
    each(4, ring_region(3), near_step)
    landed(*col, own_row(4), 0, 1)
    landed(*col, par_row(4), 3, 4, 0, 1)
    each(2, lambda i: 2 * zat(4) + i, near_step)

    for q in range(3):
        sqbuf[3 * c + q] = acc[q].astype(jnp.bfloat16)
    sq.begin()
    acc[...] = jnp.zeros_like(acc)

    def own_chip(step):
        return lambda i: (xhi * 4 + yat(step)) * 2 + i

    sq.sibling(0)
    each(2, lambda i: (xhi * 4 + y) * 2 + i, far_step)
    sq.y_near_first()
    sq.x_hop()
    sq.y_near_own()
    sq.x_late(0)
    sq.sibling(0, own_xhi=False)
    each(2, lambda i: (xhi2 * 4 + y) * 2 + i, far_step)
    sq.sibling(1)
    sq.sibling(-1)
    each(4, lambda i: (xhi * 4 + yat(1 - 2 * (i // 2))) * 2 + i % 2, far_step)
    sq.y_near_par()
    sq.x_late(1, -1)
    sq.y_far_first()
    sq.sibling(1, own_xhi=False)
    sq.sibling(-1, own_xhi=False)
    each(4, lambda i: (xhi2 * 4 + yat(1 - 2 * (i // 2))) * 2 + i % 2, far_step)
    sq.y_far()
    sq.x_last()
    each(2, lambda i: ((xhi + i) % 2 * 4 + yat(2)) * 2 + core, far_step)
    sq.sibling(2)
    sq.sibling(2, own_xhi=False)
    each(2, lambda i: ((xhi + i) % 2 * 4 + yat(2)) * 2 + core2, far_step)

    stage[3] = zero
    for q in range(3):
        stage[q] = sqbuf[3 * c + q]
    for s in range(3):
        place = jnp.minimum(rank[s], 2)
        value = 3.0 * stage[place].astype(jnp.float32) - 2.0 * acc[place]
        out[s] = jnp.where(live[s], value, 0.0).astype(jnp.bfloat16)

    for copy in started:
        copy.wait_send()


def local(tiles, stack, mask):
    vmem = pl.BlockSpec(memory_space=pltpu.VMEM)
    smem = pl.BlockSpec(memory_space=pltpu.SMEM)
    result = pl.pallas_call(
        kernel,
        out_shape=jax.ShapeDtypeStruct((3, BS, BS), jnp.bfloat16),
        in_specs=[vmem, smem, smem],
        out_specs=vmem,
        scratch_shapes=[
            pltpu.VMEM((49, BS, BS), jnp.bfloat16),
            pltpu.VMEM((48, BS, BS), jnp.bfloat16),
            pltpu.VMEM((48, BS, BS), jnp.bfloat16),
            pltpu.VMEM((4, BS, BS), jnp.bfloat16),
            pltpu.VMEM((3, BS, BS), jnp.float32),
            pltpu.SMEM((16, 9), jnp.int32),
            pltpu.SMEM((16, 9), jnp.int32),
            pltpu.SemaphoreType.DMA((SENDS,)),
            pltpu.SemaphoreType.DMA((64,)),
            pltpu.SemaphoreType.DMA((64,)),
            pltpu.SemaphoreType.DMA((64,)),
        ],
        compiler_params=pltpu.CompilerParams(
            collective_id=0, has_side_effects=True, vmem_limit_bytes=40 * 1024 * 1024
        ),
        name="purify",
    )(tiles[0, 0], stack, mask)
    return result[None, None]


def solution(mesh):
    placed = (P("row", "col", None, None, None), P("row", "col", None), P())
    return jax.shard_map(
        local,
        mesh=mesh,
        in_specs=placed,
        out_specs=P("row", "col", None, None, None),
        check_vma=False,
    )
```

```python
import jax
import jax.numpy as jnp
from jax import lax
from jax.experimental import pallas as pl
from jax.experimental.pallas import tpu as pltpu
from jax.sharding import PartitionSpec as P

MESH = pl.DeviceIdType.MESH
BS = 256
LANES = 128
REGION = 3 * BS
NAMES = 72
X_ROWS = 448
Y_ROWS = 320


def device(z, xlo, xhi, y, core):
    return (z * 2 + xlo, (xhi * 4 + y) * 2 + core)


def kernel(
    tiles_in, stack_in, mask_in, out,
    tiles, stack, mask, colbuf, rowbuf, sqbuf, stage, far_stage, near_acc, acc, meets,
    in_sem, send_sem, recv_sem,
):
    r = lax.axis_index("row")
    c = lax.axis_index("col")
    z, xlo = r // 2, r % 2
    xhi, y, core = c // 8, (c // 2) % 4, c % 2
    sign = 1 - 2 * core
    xlo2, xhi2, core2 = 1 - xlo, 1 - xhi, 1 - core

    def zat(steps):
        return (z + sign * steps + 8) % 8

    def yat(steps):
        return (y + steps + 4) % 4

    to_za = device(zat(1), xlo, xhi, y, core)
    to_zb = device(zat(-1), xlo, xhi, y, core)
    to_yc = device(z, xlo, xhi, yat(1), core)
    to_yd = device(z, xlo, xhi, yat(-1), core)
    to_xlo = device(z, xlo2, xhi, y, core)
    to_xhi = device(z, xlo, xhi2, y, core)
    to_core = device(z, xlo, xhi, y, core2)
    peers = (to_za, to_zb, to_yc, to_yd, to_xlo, to_xhi, to_core)

    barrier = pltpu.get_barrier_semaphore()
    for peer in peers:
        pl.semaphore_signal(barrier, inc=1, device_id=peer, device_id_type=MESH)
    loads = [
        pltpu.make_async_copy(mask_in, mask, in_sem.at[0]),
        pltpu.make_async_copy(stack_in, stack, in_sem.at[1]),
        pltpu.make_async_copy(tiles_in, tiles.at[pl.ds(0, 3)], in_sem.at[2]),
    ]
    for load in loads:
        load.start()
    zero = jnp.zeros((BS, BS), jnp.bfloat16)
    stage[3] = zero[:, :LANES]
    for half in range(2):
        far_stage[half, 3] = zero[:LANES]
    near_acc[...] = jnp.zeros_like(near_acc)
    acc[...] = jnp.zeros_like(acc)
    for load in loads:
        load.wait()

    def rows_of(place, first=0, count=BS):
        return pl.ds(pl.multiple_of(place * BS + first, 16), count)

    ids = [stack[0, 0, s] for s in range(3)]
    live = [mask[4 * r + ids[s] // 4, 4 * c + ids[s] % 4] > 0 for s in range(3)]
    rank = []
    for s in range(3):
        below = jnp.int32(0)
        for t in range(3):
            if t != s:
                below = below + jnp.where(live[t] & (ids[t] < ids[s]), 1, 0)
        rank.append(jnp.where(live[s], below, 3))
    own_ids = []
    for q in range(3):
        place = jnp.int32(0)
        own_id = jnp.int32(-1)
        for s in range(3):
            place = jnp.where(rank[s] == q, s, place)
            own_id = jnp.where(rank[s] == q, ids[s], own_id)
        own_ids.append(own_id)
        tile = tiles[place]
        colbuf[rows_of(3 * r + q)] = tile
        rowbuf[rows_of(3 * c + q)] = tile

    pl.semaphore_wait(barrier, len(peers))

    recv_names, panels = {}, {}

    class Panel:
        def __init__(self, buf, half, units):
            self.buf, self.half, self.units = buf, half, units
            self.tag = len(panels)
            panels[self.tag] = self
            self.sent = 0

        def block(self, rows):
            if self.half is None:
                return self.buf.at[rows]
            return self.buf.at[rows, pl.ds(self.half * LANES, LANES)]

        def copy(self, ref, name, target):
            index = recv_names.setdefault((self.tag, *name), len(recv_names))
            return pltpu.make_async_remote_copy(
                src_ref=ref, dst_ref=ref, send_sem=send_sem.at[self.tag],
                recv_sem=recv_sem.at[index], device_id=target, device_id_type=MESH,
            )

        def send(self, region, unit, name, *targets):
            first, count = self.units[unit]
            ref = self.block(rows_of(3 * region, first, count))
            self.last = name
            for target in targets:
                self.copy(ref, name, target).start()
                self.sent += count

        def landed(self, name, count):
            self.copy(self.block(pl.ds(0, count)), name, to_core).wait_recv()

        def drain(self):
            self.copy(self.block(pl.ds(0, self.sent)), self.last, to_core).wait_send()

    def own_row(steps):
        return 2 * zat(steps) + xlo

    def par_row(steps):
        return 2 * zat(steps) + xlo2

    z_rows = REGION - X_ROWS
    col_units = {
        "x": (0, X_ROWS),
        "z": (X_ROWS, z_rows),
        "z0": (X_ROWS, z_rows // 2),
        "z1": (X_ROWS + z_rows // 2, z_rows // 2),
    }

    class Column(Panel):
        def __init__(self, half, groups):
            super().__init__(colbuf, half, col_units)
            self.groups = groups

        def cross(self, region, steps):
            self.send(region, "z", ("cross", self.groups[abs(steps)]), to_xlo)

        def begin(self, *targets):
            self.send(r, "z", (1, "z"), *targets)

        def begin_x(self):
            self.send(r, "x", (1, "own"), to_za, to_zb)

        def cross_x(self):
            self.send(r, "x", ("x",), to_xlo)

        def cross_z(self):
            self.cross(r, 0)

        def partner(self):
            self.landed(("x",), X_ROWS)
            self.send(par_row(0), "x", (1, "other"), to_za, to_zb)

        def z_first(self, steps):
            self.landed((steps, "z"), 2 * z_rows)
            for way, target, part in ((-1, to_za, "z0"), (1, to_zb, "z1")):
                region = own_row(way * steps)
                self.send(region, part if steps == 3 else "z", (steps + 1, "z"), target)
            for way in (-1, 1):
                self.cross(own_row(way * steps), steps)

        def own(self, steps):
            self.landed((steps, "own"), 2 * X_ROWS)
            if steps < 3:
                self.send(own_row(-steps), "x", (steps + 1, "own"), to_za)
                self.send(own_row(steps), "x", (steps + 1, "own"), to_zb)
            else:
                self.send(own_row(-steps), "x", (4, "x"), to_za)

        def other(self, steps):
            self.landed((steps, "other"), 2 * X_ROWS)
            if steps < 3:
                self.send(par_row(-steps), "x", (steps + 1, "other"), to_za)
                self.send(par_row(steps), "x", (steps + 1, "other"), to_zb)
            else:
                self.send(par_row(steps), "x", (4, "x"), to_zb)

        def far_first(self):
            self.landed((4, "z"), z_rows)
            self.cross(own_row(4), 4)

        def far(self):
            self.landed((4, "x"), 2 * X_ROWS)

        def crossed(self, group):
            regions = sum((1, 2, 2, 2, 1)[d] for d in range(5) if self.groups[d] == group)
            self.landed(("cross", group), regions * z_rows)

    def cat(steps, own_xhi=True):
        return ((xhi if own_xhi else xhi2) * 4 + yat(steps)) * 2 + core

    class Row(Panel):
        def __init__(self, buf, half, x_first, y_first, groups):
            units = dict(enumerate(x_first))
            self.xf = list(units)
            self.groups = groups
            self.y_rows = 0
            if y_first:
                first, count = y_first
                self.y_rows = count
                units["y"] = (first, count)
                units["y0"] = (first, count // 2)
                units["y1"] = (first + count // 2, count // 2)
            super().__init__(buf, half, units)

        def share(self, steps, unit, own_xhi=True):
            group = self.groups[abs(steps), own_xhi]
            self.send(cat(steps, own_xhi), unit, ("sib", group), to_core)

        def sibling(self, group):
            regions = sum(2 if s == 1 else 1 for (s, _), g in self.groups.items() if g == group)
            self.landed(("sib", group), regions * REGION)

        def begin(self):
            me = cat(0)
            for u in self.xf:
                self.share(0, u)
                self.send(me, u, ("hop", u), to_xhi)
            if self.y_rows:
                self.send(me, "y", ("first",), to_yc, to_yd)
                self.send(me, "y", ("late", 0), to_xhi)
                self.share(0, "y")
            for u in self.xf:
                self.send(me, u, ("near", u), to_yc, to_yd)

        def x_hop(self, u):
            self.landed(("hop", u), self.units[u][1])
            self.send(cat(0, False), u, ("par", u), to_yc, to_yd)
            self.share(0, u, False)

        def y_near_first(self):
            self.landed(("first",), 2 * self.y_rows)
            self.send(cat(-1), "y0", ("ff",), to_yc)
            self.send(cat(1), "y1", ("ff",), to_yd)
            for way in (-1, 1):
                self.send(cat(way), "y", ("late", 1), to_xhi)
                self.share(way, "y")

        def y_near_own(self, u):
            self.landed(("near", u), 2 * self.units[u][1])
            self.send(cat(-1), u, ("far", u), to_yc)
            self.share(-1, u)
            self.share(1, u)

        def y_near_par(self, u):
            self.landed(("par", u), 2 * self.units[u][1])
            self.send(cat(1, False), u, ("far", u), to_yd)
            self.share(-1, u, False)
            self.share(1, u, False)

        def x_late(self, step):
            self.landed(("late", step), self.y_rows * (2 if step == 1 else 1))
            self.share(step, "y", False)
            if step == 1:
                self.share(-1, "y", False)

        def y_far_first(self):
            self.landed(("ff",), self.y_rows)
            self.send(cat(2), "y", ("late", 2), to_xhi)
            self.share(2, "y")

        def y_far(self, u):
            self.landed(("far", u), 2 * self.units[u][1])
            self.share(2, u)
            self.share(2, u, False)

    both = [(0, REGION // 2), (REGION // 2, REGION // 2)]
    thirds = [(s * BS, BS) for s in range(3)]
    rest = (REGION - Y_ROWS) // 2
    spots = [(s, o) for s in (0, 1, 2) for o in (True, False)]
    a = Column(0, [0, 0, 0, 0, 0])
    b = Column(1, [0, 0, 2, 3, 4])
    row = Row(rowbuf, None, thirds, None, {k: k[0] // 2 for k in spots})
    sq0 = Row(
        sqbuf, 0, both, None,
        {(0, True): 2, (0, False): 2, (1, True): 2, (1, False): 0, (2, True): 1, (2, False): 1},
    )
    sq1 = Row(
        sqbuf, 1, [(Y_ROWS, rest), (Y_ROWS + rest, rest)], (0, Y_ROWS),
        {(0, True): 0, (0, False): 1, (1, True): 2, (1, False): 3, (2, True): 4, (2, False): 4},
    )

    a.cross_x()
    a.begin(to_za, to_zb)
    a.begin_x()
    row.begin()
    a.cross_z()

    def table(p, carry):
        left = [jnp.int32(-1)] * 3
        count = jnp.int32(0)
        for b in range(16):
            here = mask[4 * r + b // 4, 4 * p + b % 4] > 0
            for l in range(3):
                left[l] = jnp.where(here & (count == l), b, left[l])
            count = count + jnp.where(here, 1, 0)
        count = jnp.int32(0)
        places = []
        for b in range(16):
            here = mask[4 * p + b // 4, 4 * c + b % 4] > 0
            places.append(jnp.where(here, count, 3))
            count = count + jnp.where(here, 1, 0)
        for q in range(3):
            own = own_ids[q]
            column = [jnp.int32(3)] * 4
            for kk in range(4):
                for b in range(4):
                    column[kk] = jnp.where(own % 4 == b, places[4 * kk + b], column[kk])
            for l in range(3):
                found = jnp.int32(3)
                for kk in range(4):
                    found = jnp.where(left[l] % 4 == kk, column[kk], found)
                good = (own >= 0) & (left[l] >= 0) & (left[l] // 4 == own // 4)
                found = jnp.where(good, found, 3)
                meets[p, 3 * q + l] = found
        return carry

    lax.fori_loop(0, 8, table, 0)

    def near_step(half):
        def step(p):
            for s in range(3):
                stage[s] = colbuf[rows_of(3 * p + s), half * LANES : (half + 1) * LANES]
            total = near_acc[half]
            for l in range(3):
                right = jnp.concatenate(
                    [stage[meets[p, 3 * q + l]] for q in range(3)], axis=1
                )
                total = total + jnp.dot(
                    rowbuf[rows_of(3 * p + l)], right, preferred_element_type=jnp.float32
                )
            near_acc[half] = total

        return step

    def far_step(half):
        def step(p):
            for s in range(3):
                far_stage[half, s] = colbuf[rows_of(3 * p + s, half * LANES, LANES)]
            left = jnp.concatenate(
                [
                    sqbuf[rows_of(3 * p + l), half * LANES : (half + 1) * LANES]
                    for l in range(3)
                ],
                axis=1,
            )
            for q in range(3):
                right = jnp.concatenate(
                    [far_stage[half, meets[p, 3 * q + l]] for l in range(3)], axis=0
                )
                acc[q] += jnp.dot(left, right, preferred_element_type=jnp.float32)

        return step

    def far_whole(p):
        for half in range(2):
            for s in range(3):
                far_stage[half, s] = colbuf[rows_of(3 * p + s, half * LANES, LANES)]
        for q in range(3):
            total = acc[q]
            for l in range(3):
                place = meets[p, 3 * q + l]
                right = jnp.concatenate([far_stage[0, place], far_stage[1, place]], axis=0)
                total = total + jnp.dot(
                    sqbuf[rows_of(3 * p + l)], right, preferred_element_type=jnp.float32
                )
            acc[q] = total

    def each(count, where, step):
        def body(i, carry):
            step(where(i))
            return carry

        lax.fori_loop(0, count, body, 0)

    def ring_region(steps):
        return lambda i: 2 * zat((1 - 2 * (i // 2)) * steps) + i % 2

    def square_out(half):
        for q in range(3):
            sqbuf[rows_of(3 * c + q), half * LANES : (half + 1) * LANES] = near_acc[
                half, :, q * LANES : (q + 1) * LANES
            ].astype(jnp.bfloat16)

    def chips_at(step):
        return lambda i: ((i // 2) * 4 + yat(step)) * 2 + i % 2

    a.z_first(1)
    a.partner()
    row.y_near_own(0)
    a.own(1)
    lax.fori_loop(8, 16, table, 0)
    row.x_hop(0)
    a.other(1)
    row.x_hop(1)
    a.z_first(2)
    a.own(2)
    row.x_hop(2)
    row.y_near_own(1)
    row.y_near_own(2)
    a.other(2)
    row.y_near_par(0)
    a.z_first(3)
    row.y_near_par(1)
    a.own(3)
    b.begin(to_zb)
    row.y_near_par(2)
    a.other(3)
    b.begin(to_za)
    b.begin_x()
    row.y_far(0)
    a.far_first()
    b.cross_x()
    b.cross_z()
    row.y_far(1)
    a.far()
    b.z_first(1)
    row.sibling(0)
    a.crossed(0)
    each(4, chips_at(0), near_step(0))
    b.partner()
    row.y_far(2)
    each(4, chips_at(1), near_step(0))
    b.own(1)
    b.z_first(2)
    each(4, chips_at(-1), near_step(0))
    row.sibling(1)
    each(4, chips_at(2), near_step(0))
    square_out(0)
    sq0.begin()
    b.other(1)
    b.crossed(0)
    each(6, lambda i: 2 * zat((i // 2 + 1) % 3 - 1) + i % 2, near_step(1))
    b.own(2)
    b.z_first(3)
    sq0.x_hop(0)
    sq0.y_near_own(0)
    b.other(2)
    sq0.x_hop(1)
    sq0.y_near_own(1)
    b.own(3)
    b.far_first()
    b.crossed(2)
    each(2, lambda i: 2 * zat(2) + i, near_step(1))
    sq0.y_near_par(0)
    each(2, lambda i: 2 * zat(-2) + i, near_step(1))
    b.other(3)
    sq0.y_near_par(1)
    b.crossed(3)
    each(4, ring_region(3), near_step(1))
    sq0.y_far(0)
    b.far()
    b.crossed(4)
    each(2, lambda i: 2 * zat(4) + i, near_step(1))
    square_out(1)
    sq1.begin()

    sq0.y_far(1)
    sq0.sibling(0)
    each(4, lambda i: (xhi2 * 4 + yat(1 - 2 * (i // 2))) * 2 + i % 2, far_step(0))
    sq0.sibling(1)
    each(4, chips_at(2), far_step(0))
    sq1.y_near_first()
    sq1.x_hop(0)
    sq1.y_near_own(0)
    sq1.x_hop(1)
    sq1.y_near_own(1)
    sq0.sibling(2)
    sq1.sibling(0)
    each(2, lambda i: (xhi * 4 + y) * 2 + i, far_whole)
    sq1.y_far_first()
    sq1.x_late(0)
    sq1.y_near_par(0)
    sq1.sibling(2)
    each(2, lambda i: (xhi * 4 + yat(1)) * 2 + i, far_whole)
    sq1.y_near_par(1)
    sq1.x_late(1)
    each(2, lambda i: (xhi * 4 + yat(-1)) * 2 + i, far_whole)
    sq1.y_far(0)
    sq1.sibling(1)
    each(2, lambda i: (xhi2 * 4 + y) * 2 + i, far_whole)
    sq1.y_far(1)
    sq1.x_late(2)
    sq1.sibling(3)
    each(4, lambda i: (xhi2 * 4 + yat(1 - 2 * (i // 2))) * 2 + i % 2, far_step(1))
    each(2, lambda i: (i * 4 + yat(2)) * 2 + core, far_step(1))
    sq1.sibling(4)
    each(2, lambda i: (i * 4 + yat(2)) * 2 + core2, far_step(1))

    tiles[3] = zero
    for q in range(3):
        value = 3.0 * sqbuf[rows_of(3 * c + q)].astype(jnp.float32) - 2.0 * acc[q]
        tiles[q] = value.astype(jnp.bfloat16)
    for s in range(3):
        out[s] = tiles[rank[s]]

    for panel in panels.values():
        panel.drain()


def local(tiles, stack, mask):
    hbm = pl.BlockSpec(memory_space=pltpu.HBM)
    result = pl.pallas_call(
        kernel,
        out_shape=jax.ShapeDtypeStruct((3, BS, BS), jnp.bfloat16),
        in_specs=[hbm, hbm, hbm],
        out_specs=pl.BlockSpec(memory_space=pltpu.VMEM),
        scratch_shapes=[
            pltpu.VMEM((4, BS, BS), jnp.bfloat16),
            pltpu.SMEM((1, 1, 3), jnp.int32),
            pltpu.SMEM((64, 64), jnp.int32),
            pltpu.VMEM((48 * BS, BS), jnp.bfloat16),
            pltpu.VMEM((48 * BS, BS), jnp.bfloat16),
            pltpu.VMEM((48 * BS, BS), jnp.bfloat16),
            pltpu.VMEM((4, BS, LANES), jnp.bfloat16),
            pltpu.VMEM((2, 4, LANES, BS), jnp.bfloat16),
            pltpu.VMEM((2, BS, 3 * LANES), jnp.float32),
            pltpu.VMEM((3, BS, BS), jnp.float32),
            pltpu.SMEM((16, 9), jnp.int32),
            pltpu.SemaphoreType.DMA((3,)),
            pltpu.SemaphoreType.DMA((5,)),
            pltpu.SemaphoreType.DMA((NAMES,)),
        ],
        compiler_params=pltpu.CompilerParams(
            collective_id=0, has_side_effects=True, vmem_limit_bytes=67043328
        ),
        name="purify",
    )(tiles[0, 0], stack, mask)
    return result[None, None]


def solution(mesh):
    placed = (P("row", "col", None, None, None), P("row", "col", None), P())
    return jax.shard_map(
        local,
        mesh=mesh,
        in_specs=placed,
        out_specs=P("row", "col", None, None, None),
        check_vma=False,
    )
```

```python
import jax
import jax.numpy as jnp
from jax import lax
from jax.experimental import pallas as pl
from jax.experimental.pallas import tpu as pltpu
from jax.sharding import PartitionSpec as P

MESH = pl.DeviceIdType.MESH
BS = 256
LANES = 128
REGION = 3 * BS
NAMES = 72
X_ROWS = 448
Y_ROWS = 320


def device(z, xlo, xhi, y, core):
    return (z * 2 + xlo, (xhi * 4 + y) * 2 + core)


def kernel(
    tiles_in, stack_in, mask_in, out,
    tiles, stack, mask, colbuf, rowbuf, sqbuf, stage, far_stage, near_acc, acc, meets,
    in_sem, send_sem, recv_sem,
):
    r = lax.axis_index("row")
    c = lax.axis_index("col")
    z, xlo = r // 2, r % 2
    xhi, y, core = c // 8, (c // 2) % 4, c % 2
    sign = 1 - 2 * core
    xlo2, xhi2, core2 = 1 - xlo, 1 - xhi, 1 - core

    def zat(steps):
        return (z + sign * steps + 8) % 8

    def yat(steps):
        return (y + steps + 4) % 4

    to_za = device(zat(1), xlo, xhi, y, core)
    to_zb = device(zat(-1), xlo, xhi, y, core)
    to_yc = device(z, xlo, xhi, yat(1), core)
    to_yd = device(z, xlo, xhi, yat(-1), core)
    to_xlo = device(z, xlo2, xhi, y, core)
    to_xhi = device(z, xlo, xhi2, y, core)
    to_core = device(z, xlo, xhi, y, core2)
    peers = (to_za, to_zb, to_yc, to_yd, to_xlo, to_xhi, to_core)

    barrier = pltpu.get_barrier_semaphore()
    for peer in peers:
        pl.semaphore_signal(barrier, inc=1, device_id=peer, device_id_type=MESH)
    loads = [
        pltpu.make_async_copy(mask_in, mask, in_sem.at[0]),
        pltpu.make_async_copy(stack_in, stack, in_sem.at[1]),
        pltpu.make_async_copy(tiles_in, tiles.at[pl.ds(0, 3)], in_sem.at[2]),
    ]
    for load in loads:
        load.start()
    zero = jnp.zeros((BS, BS), jnp.bfloat16)
    stage[3] = zero[:, :LANES]
    for half in range(2):
        far_stage[half, 3] = zero[:LANES]
    near_acc[...] = jnp.zeros_like(near_acc)
    acc[...] = jnp.zeros_like(acc)
    for load in loads:
        load.wait()

    def rows_of(place, first=0, count=BS):
        return pl.ds(pl.multiple_of(place * BS + first, 16), count)

    ids = [stack[0, 0, s] for s in range(3)]
    live = [mask[4 * r + ids[s] // 4, 4 * c + ids[s] % 4] > 0 for s in range(3)]
    rank = []
    for s in range(3):
        below = jnp.int32(0)
        for t in range(3):
            if t != s:
                below = below + jnp.where(live[t] & (ids[t] < ids[s]), 1, 0)
        rank.append(jnp.where(live[s], below, 3))
    own_ids = []
    for q in range(3):
        place = jnp.int32(0)
        own_id = jnp.int32(-1)
        for s in range(3):
            place = jnp.where(rank[s] == q, s, place)
            own_id = jnp.where(rank[s] == q, ids[s], own_id)
        own_ids.append(own_id)
        tile = tiles[place]
        colbuf[rows_of(3 * r + q)] = tile
        rowbuf[rows_of(3 * c + q)] = tile

    pl.semaphore_wait(barrier, len(peers))

    recv_names, panels = {}, {}

    class Panel:
        def __init__(self, buf, half, units):
            self.buf, self.half, self.units = buf, half, units
            self.tag = len(panels)
            panels[self.tag] = self
            self.sent = 0

        def block(self, rows):
            if self.half is None:
                return self.buf.at[rows]
            return self.buf.at[rows, pl.ds(self.half * LANES, LANES)]

        def copy(self, ref, name, target):
            index = recv_names.setdefault((self.tag, *name), len(recv_names))
            return pltpu.make_async_remote_copy(
                src_ref=ref, dst_ref=ref, send_sem=send_sem.at[self.tag],
                recv_sem=recv_sem.at[index], device_id=target, device_id_type=MESH,
            )

        def send(self, region, unit, name, *targets):
            first, count = self.units[unit]
            ref = self.block(rows_of(3 * region, first, count))
            self.last = name
            for target in targets:
                self.copy(ref, name, target).start()
                self.sent += count

        def landed(self, name, count):
            self.copy(self.block(pl.ds(0, count)), name, to_core).wait_recv()

        def drain(self):
            self.copy(self.block(pl.ds(0, self.sent)), self.last, to_core).wait_send()

    def own_row(steps):
        return 2 * zat(steps) + xlo

    def par_row(steps):
        return 2 * zat(steps) + xlo2

    z_rows = REGION - X_ROWS
    col_units = {
        "x": (0, X_ROWS),
        "x0": (0, X_ROWS // 2),
        "x1": (X_ROWS // 2, X_ROWS // 2),
        "z": (X_ROWS, z_rows),
        "z0": (X_ROWS, z_rows // 2),
        "z1": (X_ROWS + z_rows // 2, z_rows // 2),
    }

    class Column(Panel):
        def __init__(self, half, groups):
            super().__init__(colbuf, half, col_units)
            self.groups = groups

        def cross(self, region, steps):
            self.send(region, "z", ("cross", self.groups[abs(steps)]), to_xlo)

        def begin(self, *targets):
            self.send(r, "z", (1, "z"), *targets)

        def begin_x(self):
            self.send(r, "x", (1, "own"), to_za, to_zb)

        def cross_x(self):
            self.send(r, "x", ("x",), to_xlo)

        def cross_z(self):
            self.cross(r, 0)

        def partner(self):
            self.landed(("x",), X_ROWS)
            self.send(par_row(0), "x", (1, "other"), to_za, to_zb)

        def z_first(self, steps):
            self.landed((steps, "z"), 2 * z_rows)
            for way, target, part in ((-1, to_za, "z0"), (1, to_zb, "z1")):
                region = own_row(way * steps)
                self.send(region, part if steps == 3 else "z", (steps + 1, "z"), target)
            for way in (-1, 1):
                self.cross(own_row(way * steps), steps)

        def own(self, steps):
            self.landed((steps, "own"), 2 * X_ROWS)
            if steps < 3:
                self.send(own_row(-steps), "x", (steps + 1, "own"), to_za)
                self.send(own_row(steps), "x", (steps + 1, "own"), to_zb)
            else:
                self.send(own_row(-steps), "x", (4, "x"), to_za)

        def other(self, steps):
            self.landed((steps, "other"), 2 * X_ROWS)
            if steps < 3:
                self.send(par_row(-steps), "x", (steps + 1, "other"), to_za)
                self.send(par_row(steps), "x", (steps + 1, "other"), to_zb)
            else:
                self.send(par_row(steps), "x1", (4, "x"), to_zb)
                self.send(par_row(-steps), "x0", (4, "x"), to_za)

        def far_first(self):
            self.landed((4, "z"), z_rows)
            self.cross(own_row(4), 4)

        def far(self):
            self.landed((4, "x"), 2 * X_ROWS)

        def crossed(self, group):
            regions = sum((1, 2, 2, 2, 1)[d] for d in range(5) if self.groups[d] == group)
            self.landed(("cross", group), regions * z_rows)

    def cat(steps, own_xhi=True):
        return ((xhi if own_xhi else xhi2) * 4 + yat(steps)) * 2 + core

    class Row(Panel):
        def __init__(self, buf, half, x_first, y_first, groups):
            units = dict(enumerate(x_first))
            self.xf = list(units)
            self.groups = groups
            self.y_rows = 0
            if y_first:
                first, count = y_first
                self.y_rows = count
                units["y"] = (first, count)
                units["y0"] = (first, count // 2)
                units["y1"] = (first + count // 2, count // 2)
            super().__init__(buf, half, units)

        def share(self, steps, unit, own_xhi=True):
            group = self.groups[abs(steps), own_xhi]
            self.send(cat(steps, own_xhi), unit, ("sib", group), to_core)

        def sibling(self, group):
            regions = sum(2 if s == 1 else 1 for (s, _), g in self.groups.items() if g == group)
            self.landed(("sib", group), regions * REGION)

        def begin(self):
            me = cat(0)
            for u in self.xf:
                self.share(0, u)
                self.send(me, u, ("hop", u), to_xhi)
            if self.y_rows:
                self.send(me, "y", ("first",), to_yc, to_yd)
                self.send(me, "y", ("late", 0), to_xhi)
                self.share(0, "y")
            for u in self.xf:
                self.send(me, u, ("near", u), to_yc, to_yd)

        def x_hop(self, u):
            self.landed(("hop", u), self.units[u][1])
            self.send(cat(0, False), u, ("par", u), to_yc, to_yd)
            self.share(0, u, False)

        def y_near_first(self):
            self.landed(("first",), 2 * self.y_rows)
            self.send(cat(-1), "y0", ("ff",), to_yc)
            self.send(cat(1), "y1", ("ff",), to_yd)
            for way in (-1, 1):
                self.send(cat(way), "y", ("late", 1), to_xhi)
                self.share(way, "y")

        def y_near_own(self, u):
            self.landed(("near", u), 2 * self.units[u][1])
            self.send(cat(-1), u, ("far", u), to_yc)
            self.share(-1, u)
            self.share(1, u)

        def y_near_par(self, u):
            self.landed(("par", u), 2 * self.units[u][1])
            self.send(cat(1, False), u, ("far", u), to_yd)
            self.share(-1, u, False)
            self.share(1, u, False)

        def x_late(self, step):
            self.landed(("late", step), self.y_rows * (2 if step == 1 else 1))
            self.share(step, "y", False)
            if step == 1:
                self.share(-1, "y", False)

        def y_far_first(self):
            self.landed(("ff",), self.y_rows)
            self.send(cat(2), "y", ("late", 2), to_xhi)
            self.share(2, "y")

        def y_far(self, u):
            self.landed(("far", u), 2 * self.units[u][1])
            self.share(2, u)
            self.share(2, u, False)

    both = [(0, REGION // 2), (REGION // 2, REGION // 2)]
    thirds = [(s * BS, BS) for s in range(3)]
    rest = (REGION - Y_ROWS) // 2
    spots = [(s, o) for s in (0, 1, 2) for o in (True, False)]
    a = Column(0, [0, 0, 0, 0, 0])
    b = Column(1, [0, 0, 2, 3, 4])
    row = Row(rowbuf, None, thirds, None, {k: k[0] // 2 for k in spots})
    sq0 = Row(
        sqbuf, 0, both, None,
        {(0, True): 2, (0, False): 2, (1, True): 2, (1, False): 0, (2, True): 1, (2, False): 1},
    )
    sq1 = Row(
        sqbuf, 1, [(Y_ROWS, rest), (Y_ROWS + rest, rest)], (0, Y_ROWS),
        {(0, True): 0, (0, False): 1, (1, True): 2, (1, False): 3, (2, True): 4, (2, False): 4},
    )

    a.cross_x()
    a.begin(to_za, to_zb)
    a.begin_x()
    row.begin()
    a.cross_z()

    def table(p, carry):
        left = [jnp.int32(-1)] * 3
        count = jnp.int32(0)
        for b in range(16):
            here = mask[4 * r + b // 4, 4 * p + b % 4] > 0
            for l in range(3):
                left[l] = jnp.where(here & (count == l), b, left[l])
            count = count + jnp.where(here, 1, 0)
        count = jnp.int32(0)
        places = []
        for b in range(16):
            here = mask[4 * p + b // 4, 4 * c + b % 4] > 0
            places.append(jnp.where(here, count, 3))
            count = count + jnp.where(here, 1, 0)
        for q in range(3):
            own = own_ids[q]
            column = [jnp.int32(3)] * 4
            for kk in range(4):
                for b in range(4):
                    column[kk] = jnp.where(own % 4 == b, places[4 * kk + b], column[kk])
            for l in range(3):
                found = jnp.int32(3)
                for kk in range(4):
                    found = jnp.where(left[l] % 4 == kk, column[kk], found)
                good = (own >= 0) & (left[l] >= 0) & (left[l] // 4 == own // 4)
                found = jnp.where(good, found, 3)
                meets[p, 3 * q + l] = found
        return carry

    lax.fori_loop(0, 8, table, 0)

    def near_step(half):
        def step(p):
            for s in range(3):
                stage[s] = colbuf[rows_of(3 * p + s), half * LANES : (half + 1) * LANES]
            total = near_acc[half]
            for l in range(3):
                right = jnp.concatenate(
                    [stage[meets[p, 3 * q + l]] for q in range(3)], axis=1
                )
                total = total + jnp.dot(
                    rowbuf[rows_of(3 * p + l)], right, preferred_element_type=jnp.float32
                )
            near_acc[half] = total

        return step

    def far_step(half):
        def step(p):
            for s in range(3):
                far_stage[half, s] = colbuf[rows_of(3 * p + s, half * LANES, LANES)]
            left = jnp.concatenate(
                [
                    sqbuf[rows_of(3 * p + l), half * LANES : (half + 1) * LANES]
                    for l in range(3)
                ],
                axis=1,
            )
            for q in range(3):
                right = jnp.concatenate(
                    [far_stage[half, meets[p, 3 * q + l]] for l in range(3)], axis=0
                )
                acc[q] += jnp.dot(left, right, preferred_element_type=jnp.float32)

        return step

    def far_whole(p):
        for half in range(2):
            for s in range(3):
                far_stage[half, s] = colbuf[rows_of(3 * p + s, half * LANES, LANES)]
        for q in range(3):
            total = acc[q]
            for l in range(3):
                place = meets[p, 3 * q + l]
                right = jnp.concatenate([far_stage[0, place], far_stage[1, place]], axis=0)
                total = total + jnp.dot(
                    sqbuf[rows_of(3 * p + l)], right, preferred_element_type=jnp.float32
                )
            acc[q] = total

    def each(count, where, step):
        def body(i, carry):
            step(where(i))
            return carry

        lax.fori_loop(0, count, body, 0)

    def ring_region(steps):
        return lambda i: 2 * zat((1 - 2 * (i // 2)) * steps) + i % 2

    def square_out(half):
        for q in range(3):
            sqbuf[rows_of(3 * c + q), half * LANES : (half + 1) * LANES] = near_acc[
                half, :, q * LANES : (q + 1) * LANES
            ].astype(jnp.bfloat16)

    def chips_at(step):
        return lambda i: ((i // 2) * 4 + yat(step)) * 2 + i % 2

    a.z_first(1)
    a.partner()
    row.y_near_own(0)
    a.own(1)
    lax.fori_loop(8, 16, table, 0)
    row.x_hop(0)
    a.other(1)
    row.x_hop(1)
    a.z_first(2)
    a.own(2)
    row.x_hop(2)
    row.y_near_own(1)
    row.y_near_own(2)
    a.other(2)
    row.y_near_par(0)
    a.z_first(3)
    row.y_near_par(1)
    a.own(3)
    b.begin(to_zb)
    row.y_near_par(2)
    a.other(3)
    b.begin(to_za)
    b.begin_x()
    row.y_far(0)
    a.far_first()
    b.cross_x()
    b.cross_z()
    row.y_far(1)
    a.far()
    b.z_first(1)
    row.sibling(0)
    a.crossed(0)
    each(4, chips_at(0), near_step(0))
    b.partner()
    row.y_far(2)
    each(4, chips_at(1), near_step(0))
    b.own(1)
    b.z_first(2)
    each(4, chips_at(-1), near_step(0))
    row.sibling(1)
    each(4, chips_at(2), near_step(0))
    square_out(0)
    sq0.begin()
    b.other(1)
    b.crossed(0)
    each(6, lambda i: 2 * zat((i // 2 + 1) % 3 - 1) + i % 2, near_step(1))
    b.own(2)
    b.z_first(3)
    sq0.x_hop(0)
    sq0.y_near_own(0)
    b.other(2)
    sq0.x_hop(1)
    sq0.y_near_own(1)
    b.own(3)
    b.far_first()
    b.crossed(2)
    each(2, lambda i: 2 * zat(2) + i, near_step(1))
    sq0.y_near_par(0)
    each(2, lambda i: 2 * zat(-2) + i, near_step(1))
    b.other(3)
    sq0.y_near_par(1)
    b.crossed(3)
    each(4, ring_region(3), near_step(1))
    sq0.y_far(0)
    b.far()
    b.crossed(4)
    each(2, lambda i: 2 * zat(4) + i, near_step(1))
    square_out(1)
    sq1.begin()

    sq0.sibling(2)
    each(4, lambda i: (xhi * 4 + yat(1 - 2 * (i // 2))) * 2 + i % 2, far_step(0))
    sq0.y_far(1)
    sq0.sibling(0)
    each(4, lambda i: (xhi2 * 4 + yat(1 - 2 * (i // 2))) * 2 + i % 2, far_step(0))
    sq1.y_near_first()
    sq1.x_hop(0)
    sq1.y_near_own(0)
    sq0.sibling(1)
    each(2, lambda i: (i * 4 + yat(2)) * 2 + core, far_step(0))
    sq1.x_hop(1)
    sq1.y_near_own(1)
    each(2, lambda i: (i * 4 + yat(2)) * 2 + core2, far_step(0))
    sq1.y_far_first()
    sq1.sibling(0)
    each(2, lambda i: (xhi * 4 + y) * 2 + i, far_whole)
    sq1.x_late(0)
    sq1.y_near_par(0)
    sq1.sibling(2)
    each(2, lambda i: (xhi * 4 + yat(1)) * 2 + i, far_step(1))
    sq1.y_near_par(1)
    sq1.x_late(1)
    each(2, lambda i: (xhi * 4 + yat(-1)) * 2 + i, far_step(1))
    sq1.sibling(1)
    each(2, lambda i: (xhi2 * 4 + y) * 2 + i, far_whole)
    sq1.y_far(0)
    sq1.sibling(3)
    each(2, lambda i: (xhi2 * 4 + yat(1)) * 2 + i, far_step(1))
    sq1.y_far(1)
    sq1.x_late(2)
    each(2, lambda i: (xhi2 * 4 + yat(-1)) * 2 + i, far_step(1))
    each(2, lambda i: (i * 4 + yat(2)) * 2 + core, far_step(1))
    sq1.sibling(4)
    each(2, lambda i: (i * 4 + yat(2)) * 2 + core2, far_step(1))

    tiles[3] = zero
    for q in range(3):
        value = 3.0 * sqbuf[rows_of(3 * c + q)].astype(jnp.float32) - 2.0 * acc[q]
        tiles[q] = value.astype(jnp.bfloat16)
    for s in range(3):
        out[s] = tiles[rank[s]]

    for panel in panels.values():
        panel.drain()


def local(tiles, stack, mask):
    hbm = pl.BlockSpec(memory_space=pltpu.HBM)
    result = pl.pallas_call(
        kernel,
        out_shape=jax.ShapeDtypeStruct((3, BS, BS), jnp.bfloat16),
        in_specs=[hbm, hbm, hbm],
        out_specs=pl.BlockSpec(memory_space=pltpu.VMEM),
        scratch_shapes=[
            pltpu.VMEM((4, BS, BS), jnp.bfloat16),
            pltpu.SMEM((1, 1, 3), jnp.int32),
            pltpu.SMEM((64, 64), jnp.int32),
            pltpu.VMEM((48 * BS, BS), jnp.bfloat16),
            pltpu.VMEM((48 * BS, BS), jnp.bfloat16),
            pltpu.VMEM((48 * BS, BS), jnp.bfloat16),
            pltpu.VMEM((4, BS, LANES), jnp.bfloat16),
            pltpu.VMEM((2, 4, LANES, BS), jnp.bfloat16),
            pltpu.VMEM((2, BS, 3 * LANES), jnp.float32),
            pltpu.VMEM((3, BS, BS), jnp.float32),
            pltpu.SMEM((16, 9), jnp.int32),
            pltpu.SemaphoreType.DMA((3,)),
            pltpu.SemaphoreType.DMA((5,)),
            pltpu.SemaphoreType.DMA((NAMES,)),
        ],
        compiler_params=pltpu.CompilerParams(
            collective_id=0, has_side_effects=True, vmem_limit_bytes=67043328
        ),
        name="purify",
    )(tiles[0, 0], stack, mask)
    return result[None, None]


def solution(mesh):
    placed = (P("row", "col", None, None, None), P("row", "col", None), P())
    return jax.shard_map(
        local,
        mesh=mesh,
        in_specs=placed,
        out_specs=P("row", "col", None, None, None),
        check_vma=False,
    )
```

```python
import jax
import jax.numpy as jnp
from jax import lax
from jax.experimental import pallas as pl
from jax.experimental.pallas import tpu as pltpu
from jax.sharding import PartitionSpec as P

MESH = pl.DeviceIdType.MESH
BS = 256
LANES = 128
REGION = 3 * BS
NAMES = 76
X_ROWS = 448
Y_ROWS = 320


def device(z, xlo, xhi, y, core):
    return (z * 2 + xlo, (xhi * 4 + y) * 2 + core)


def kernel(
    tiles_in, stack_in, mask_in, out,
    tiles, stack, mask, colbuf, rowbuf, sqbuf, stage, far_stage, near_acc, acc, meets,
    in_sem, send_sem, recv_sem,
):
    r = lax.axis_index("row")
    c = lax.axis_index("col")
    z, xlo = r // 2, r % 2
    xhi, y, core = c // 8, (c // 2) % 4, c % 2
    sign = 1 - 2 * core
    xlo2, xhi2, core2 = 1 - xlo, 1 - xhi, 1 - core

    def zat(steps):
        return (z + sign * steps + 8) % 8

    def yat(steps):
        return (y + steps + 4) % 4

    to_za = device(zat(1), xlo, xhi, y, core)
    to_zb = device(zat(-1), xlo, xhi, y, core)
    to_yc = device(z, xlo, xhi, yat(1), core)
    to_yd = device(z, xlo, xhi, yat(-1), core)
    to_xlo = device(z, xlo2, xhi, y, core)
    to_xhi = device(z, xlo, xhi2, y, core)
    to_core = device(z, xlo, xhi, y, core2)
    peers = (to_za, to_zb, to_yc, to_yd, to_xlo, to_xhi, to_core)

    barrier = pltpu.get_barrier_semaphore()
    for peer in peers:
        pl.semaphore_signal(barrier, inc=1, device_id=peer, device_id_type=MESH)
    loads = [
        pltpu.make_async_copy(mask_in, mask, in_sem.at[0]),
        pltpu.make_async_copy(stack_in, stack, in_sem.at[1]),
        pltpu.make_async_copy(tiles_in, tiles.at[pl.ds(0, 3)], in_sem.at[2]),
    ]
    for load in loads:
        load.start()
    zero = jnp.zeros((BS, BS), jnp.bfloat16)
    stage[3] = zero[:, :LANES]
    for half in range(2):
        far_stage[half, 3] = zero[:LANES]
    near_acc[...] = jnp.zeros_like(near_acc)
    acc[...] = jnp.zeros_like(acc)
    for load in loads:
        load.wait()

    def rows_of(place, first=0, count=BS):
        return pl.ds(pl.multiple_of(place * BS + first, 16), count)

    ids = [stack[0, 0, s] for s in range(3)]
    live = [mask[4 * r + ids[s] // 4, 4 * c + ids[s] % 4] > 0 for s in range(3)]
    rank = []
    for s in range(3):
        below = jnp.int32(0)
        for t in range(3):
            if t != s:
                below = below + jnp.where(live[t] & (ids[t] < ids[s]), 1, 0)
        rank.append(jnp.where(live[s], below, 3))
    own_ids = []
    for q in range(3):
        place = jnp.int32(0)
        own_id = jnp.int32(-1)
        for s in range(3):
            place = jnp.where(rank[s] == q, s, place)
            own_id = jnp.where(rank[s] == q, ids[s], own_id)
        own_ids.append(own_id)
        tile = tiles[place]
        colbuf[rows_of(3 * r + q)] = tile
        rowbuf[rows_of(3 * c + q)] = tile

    pl.semaphore_wait(barrier, len(peers))

    recv_names, panels = {}, {}

    class Panel:
        def __init__(self, buf, half, units):
            self.buf, self.half, self.units = buf, half, units
            self.tag = len(panels)
            panels[self.tag] = self
            self.sent = 0

        def block(self, rows):
            if self.half is None:
                return self.buf.at[rows]
            return self.buf.at[rows, pl.ds(self.half * LANES, LANES)]

        def copy(self, ref, name, target):
            index = recv_names.setdefault((self.tag, *name), len(recv_names))
            return pltpu.make_async_remote_copy(
                src_ref=ref, dst_ref=ref, send_sem=send_sem.at[self.tag],
                recv_sem=recv_sem.at[index], device_id=target, device_id_type=MESH,
            )

        def send(self, region, unit, name, *targets):
            first, count = self.units[unit]
            ref = self.block(rows_of(3 * region, first, count))
            self.last = name
            for target in targets:
                self.copy(ref, name, target).start()
                self.sent += count

        def landed(self, name, count):
            self.copy(self.block(pl.ds(0, count)), name, to_core).wait_recv()

        def drain(self):
            self.copy(self.block(pl.ds(0, self.sent)), self.last, to_core).wait_send()

    def own_row(steps):
        return 2 * zat(steps) + xlo

    def par_row(steps):
        return 2 * zat(steps) + xlo2

    z_rows = REGION - X_ROWS
    col_units = {
        "x": (0, X_ROWS),
        "x0": (0, X_ROWS // 2),
        "x1": (X_ROWS // 2, X_ROWS // 2),
        "z": (X_ROWS, z_rows),
        "z0": (X_ROWS, z_rows // 2),
        "z1": (X_ROWS + z_rows // 2, z_rows // 2),
    }

    class Column(Panel):
        def __init__(self, half, groups):
            super().__init__(colbuf, half, col_units)
            self.groups = groups

        def cross(self, region, steps):
            self.send(region, "z", ("cross", self.groups[abs(steps)]), to_xlo)

        def begin(self, *targets):
            self.send(r, "z", (1, "z"), *targets)

        def begin_x(self):
            self.send(r, "x", (1, "own"), to_za, to_zb)

        def cross_x(self):
            self.send(r, "x", ("x",), to_xlo)

        def cross_z(self):
            self.cross(r, 0)

        def partner(self):
            self.landed(("x",), X_ROWS)
            self.send(par_row(0), "x", (1, "other"), to_za, to_zb)

        def z_first(self, steps):
            self.landed((steps, "z"), 2 * z_rows)
            for way, target, part in ((-1, to_za, "z0"), (1, to_zb, "z1")):
                region = own_row(way * steps)
                self.send(region, part if steps == 3 else "z", (steps + 1, "z"), target)
            for way in (-1, 1):
                self.cross(own_row(way * steps), steps)

        def own(self, steps):
            self.landed((steps, "own"), 2 * X_ROWS)
            if steps < 3:
                self.send(own_row(-steps), "x", (steps + 1, "own"), to_za)
                self.send(own_row(steps), "x", (steps + 1, "own"), to_zb)
            else:
                self.send(own_row(-steps), "x", (4, "x"), to_za)

        def other(self, steps):
            self.landed((steps, "other"), 2 * X_ROWS)
            if steps < 3:
                self.send(par_row(-steps), "x", (steps + 1, "other"), to_za)
                self.send(par_row(steps), "x", (steps + 1, "other"), to_zb)
            else:
                self.send(par_row(steps), "x1", (4, "x"), to_zb)
                self.send(par_row(-steps), "x0", (4, "x"), to_za)

        def far_first(self):
            self.landed((4, "z"), z_rows)
            self.cross(own_row(4), 4)

        def far(self):
            self.landed((4, "x"), 2 * X_ROWS)

        def crossed(self, group):
            regions = sum((1, 2, 2, 2, 1)[d] for d in range(5) if self.groups[d] == group)
            self.landed(("cross", group), regions * z_rows)

    def cat(steps, own_xhi=True):
        return ((xhi if own_xhi else xhi2) * 4 + yat(steps)) * 2 + core

    class Row(Panel):
        def __init__(self, buf, half, x_first, y_first, groups):
            units = dict(enumerate(x_first))
            self.xf = list(units)
            self.groups = groups
            self.y_rows = 0
            if y_first:
                first, count = y_first
                self.y_rows = count
                units["y"] = (first, count)
                units["y0"] = (first, count // 2)
                units["y1"] = (first + count // 2, count // 2)
            super().__init__(buf, half, units)

        def share(self, steps, unit, own_xhi=True):
            group = self.groups[abs(steps), own_xhi]
            self.send(cat(steps, own_xhi), unit, ("sib", group), to_core)

        def sibling(self, group):
            regions = sum(2 if s == 1 else 1 for (s, _), g in self.groups.items() if g == group)
            self.landed(("sib", group), regions * REGION)

        def begin(self):
            me = cat(0)
            for u in self.xf:
                self.share(0, u)
                self.send(me, u, ("hop", u), to_xhi)
            if self.y_rows:
                self.send(me, "y", ("first",), to_yc, to_yd)
                self.send(me, "y", ("late", 0), to_xhi)
                self.share(0, "y")
            for u in self.xf:
                self.send(me, u, ("near", u), to_yc, to_yd)

        def x_hop(self, u):
            self.landed(("hop", u), self.units[u][1])
            self.send(cat(0, False), u, ("par", u), to_yc, to_yd)
            self.share(0, u, False)

        def y_near_first(self):
            self.landed(("first",), 2 * self.y_rows)
            self.send(cat(-1), "y0", ("ff",), to_yc)
            self.send(cat(1), "y1", ("ff",), to_yd)
            for way in (-1, 1):
                self.send(cat(way), "y", ("late", 1), to_xhi)
                self.share(way, "y")

        def y_near_own(self, u):
            self.landed(("near", u), 2 * self.units[u][1])
            self.send(cat(-1), u, ("far", u), to_yc)
            self.share(-1, u)
            self.share(1, u)

        def y_near_par(self, u):
            self.landed(("par", u), 2 * self.units[u][1])
            self.send(cat(1, False), u, ("far", u), to_yd)
            self.share(-1, u, False)
            self.share(1, u, False)

        def x_late(self, step):
            self.landed(("late", step), self.y_rows * (2 if step == 1 else 1))
            self.share(step, "y", False)
            if step == 1:
                self.share(-1, "y", False)

        def y_far_first(self):
            self.landed(("ff",), self.y_rows)
            self.send(cat(2), "y", ("late", 2), to_xhi)
            self.share(2, "y")

        def y_far(self, u):
            self.landed(("far", u), 2 * self.units[u][1])
            self.share(2, u)
            self.share(2, u, False)

    both = [(0, REGION // 2), (REGION // 2, REGION // 2)]
    thirds = [(s * BS, BS) for s in range(3)]
    spots = [(s, o) for s in (0, 1, 2) for o in (True, False)]
    a = Column(0, [0, 0, 0, 0, 0])
    b = Column(1, [0, 0, 2, 3, 4])
    row = Row(rowbuf, None, thirds, None, {k: k[0] // 2 for k in spots})
    sq0 = Row(
        sqbuf, 0, both, None,
        {(0, True): 2, (0, False): 2, (1, True): 2, (1, False): 0, (2, True): 1, (2, False): 1},
    )
    sq1 = Row(
        sqbuf, 1, [(320, 160), (480, 144), (624, 144)], (0, Y_ROWS),
        {(0, True): 0, (0, False): 1, (1, True): 2, (1, False): 3, (2, True): 4, (2, False): 4},
    )

    a.cross_x()
    a.begin(to_za, to_zb)
    a.begin_x()
    row.begin()
    a.cross_z()

    def table(p, carry):
        left = [jnp.int32(-1)] * 3
        count = jnp.int32(0)
        for b in range(16):
            here = mask[4 * r + b // 4, 4 * p + b % 4] > 0
            for l in range(3):
                left[l] = jnp.where(here & (count == l), b, left[l])
            count = count + jnp.where(here, 1, 0)
        count = jnp.int32(0)
        places = []
        for b in range(16):
            here = mask[4 * p + b // 4, 4 * c + b % 4] > 0
            places.append(jnp.where(here, count, 3))
            count = count + jnp.where(here, 1, 0)
        for q in range(3):
            own = own_ids[q]
            column = [jnp.int32(3)] * 4
            for kk in range(4):
                for b in range(4):
                    column[kk] = jnp.where(own % 4 == b, places[4 * kk + b], column[kk])
            for l in range(3):
                found = jnp.int32(3)
                for kk in range(4):
                    found = jnp.where(left[l] % 4 == kk, column[kk], found)
                good = (own >= 0) & (left[l] >= 0) & (left[l] // 4 == own // 4)
                found = jnp.where(good, found, 3)
                meets[p, 3 * q + l] = found
        return carry

    lax.fori_loop(0, 8, table, 0)

    def near_step(half):
        def step(p):
            for s in range(3):
                stage[s] = colbuf[rows_of(3 * p + s), half * LANES : (half + 1) * LANES]
            total = near_acc[half]
            for l in range(3):
                right = jnp.concatenate(
                    [stage[meets[p, 3 * q + l]] for q in range(3)], axis=1
                )
                total = total + jnp.dot(
                    rowbuf[rows_of(3 * p + l)], right, preferred_element_type=jnp.float32
                )
            near_acc[half] = total

        return step

    def far_step(half):
        def step(p):
            for s in range(3):
                far_stage[half, s] = colbuf[rows_of(3 * p + s, half * LANES, LANES)]
            left = jnp.concatenate(
                [
                    sqbuf[rows_of(3 * p + l), half * LANES : (half + 1) * LANES]
                    for l in range(3)
                ],
                axis=1,
            )
            for q in range(3):
                right = jnp.concatenate(
                    [far_stage[half, meets[p, 3 * q + l]] for l in range(3)], axis=0
                )
                acc[q] += jnp.dot(left, right, preferred_element_type=jnp.float32)

        return step

    def far_whole(p):
        for half in range(2):
            for s in range(3):
                far_stage[half, s] = colbuf[rows_of(3 * p + s, half * LANES, LANES)]
        for q in range(3):
            total = acc[q]
            for l in range(3):
                place = meets[p, 3 * q + l]
                right = jnp.concatenate([far_stage[0, place], far_stage[1, place]], axis=0)
                total = total + jnp.dot(
                    sqbuf[rows_of(3 * p + l)], right, preferred_element_type=jnp.float32
                )
            acc[q] = total

    def each(count, where, step):
        def body(i, carry):
            step(where(i))
            return carry

        lax.fori_loop(0, count, body, 0)

    def ring_region(steps):
        return lambda i: 2 * zat((1 - 2 * (i // 2)) * steps) + i % 2

    def square_out(half):
        for q in range(3):
            sqbuf[rows_of(3 * c + q), half * LANES : (half + 1) * LANES] = near_acc[
                half, :, q * LANES : (q + 1) * LANES
            ].astype(jnp.bfloat16)

    def chips_at(step):
        return lambda i: ((i // 2) * 4 + yat(step)) * 2 + i % 2

    a.z_first(1)
    a.partner()
    row.y_near_own(0)
    a.own(1)
    lax.fori_loop(8, 16, table, 0)
    row.x_hop(0)
    a.other(1)
    row.x_hop(1)
    a.z_first(2)
    a.own(2)
    row.x_hop(2)
    row.y_near_own(1)
    row.y_near_own(2)
    a.other(2)
    row.y_near_par(0)
    a.z_first(3)
    row.y_near_par(1)
    a.own(3)
    b.begin(to_zb)
    row.y_near_par(2)
    a.other(3)
    b.begin(to_za)
    b.begin_x()
    row.y_far(0)
    a.far_first()
    b.cross_x()
    b.cross_z()
    row.y_far(1)
    a.far()
    b.z_first(1)
    row.sibling(0)
    a.crossed(0)
    each(4, chips_at(0), near_step(0))
    b.partner()
    row.y_far(2)
    each(4, chips_at(1), near_step(0))
    b.own(1)
    b.z_first(2)
    each(4, chips_at(-1), near_step(0))
    row.sibling(1)
    each(4, chips_at(2), near_step(0))
    square_out(0)
    sq0.begin()
    b.other(1)
    b.crossed(0)
    each(6, lambda i: 2 * zat((i // 2 + 1) % 3 - 1) + i % 2, near_step(1))
    b.own(2)
    b.z_first(3)
    sq0.x_hop(0)
    sq0.y_near_own(0)
    b.other(2)
    sq0.x_hop(1)
    sq0.y_near_own(1)
    b.own(3)
    b.far_first()
    b.crossed(2)
    each(2, lambda i: 2 * zat(2) + i, near_step(1))
    sq0.y_near_par(0)
    each(2, lambda i: 2 * zat(-2) + i, near_step(1))
    b.other(3)
    sq0.y_near_par(1)
    b.crossed(3)
    each(4, ring_region(3), near_step(1))
    sq0.y_far(0)
    b.far()
    b.crossed(4)
    each(2, lambda i: 2 * zat(4) + i, near_step(1))
    square_out(1)
    sq1.begin()

    sq0.sibling(2)
    each(4, lambda i: (xhi * 4 + yat(1 - 2 * (i // 2))) * 2 + i % 2, far_step(0))
    sq0.y_far(1)
    sq0.sibling(0)
    each(4, lambda i: (xhi2 * 4 + yat(1 - 2 * (i // 2))) * 2 + i % 2, far_step(0))
    sq1.y_near_first()
    sq1.x_hop(0)
    sq1.y_near_own(0)
    sq1.x_hop(1)
    sq0.sibling(1)
    each(2, lambda i: (i * 4 + yat(2)) * 2 + core, far_step(0))
    sq1.x_hop(2)
    sq1.y_near_own(1)
    sq1.y_near_own(2)
    each(2, lambda i: (i * 4 + yat(2)) * 2 + core2, far_step(0))
    sq1.y_far_first()
    sq1.sibling(0)
    each(2, lambda i: (xhi * 4 + y) * 2 + i, far_whole)
    sq1.x_late(0)
    sq1.y_near_par(0)
    sq1.sibling(2)
    each(2, lambda i: (xhi * 4 + yat(1)) * 2 + i, far_step(1))
    sq1.y_near_par(1)
    sq1.y_near_par(2)
    sq1.x_late(1)
    each(2, lambda i: (xhi * 4 + yat(-1)) * 2 + i, far_step(1))
    sq1.sibling(1)
    each(2, lambda i: (xhi2 * 4 + y) * 2 + i, far_whole)
    sq1.y_far(0)
    sq1.sibling(3)
    each(2, lambda i: (xhi2 * 4 + yat(1)) * 2 + i, far_step(1))
    sq1.y_far(1)
    sq1.y_far(2)
    sq1.x_late(2)
    each(2, lambda i: (xhi2 * 4 + yat(-1)) * 2 + i, far_step(1))
    each(2, lambda i: (i * 4 + yat(2)) * 2 + core, far_step(1))
    sq1.sibling(4)
    each(2, lambda i: (i * 4 + yat(2)) * 2 + core2, far_step(1))

    tiles[3] = zero
    for q in range(3):
        value = 3.0 * sqbuf[rows_of(3 * c + q)].astype(jnp.float32) - 2.0 * acc[q]
        tiles[q] = value.astype(jnp.bfloat16)
    for s in range(3):
        out[s] = tiles[rank[s]]

    for panel in panels.values():
        panel.drain()


def local(tiles, stack, mask):
    hbm = pl.BlockSpec(memory_space=pltpu.HBM)
    result = pl.pallas_call(
        kernel,
        out_shape=jax.ShapeDtypeStruct((3, BS, BS), jnp.bfloat16),
        in_specs=[hbm, hbm, hbm],
        out_specs=pl.BlockSpec(memory_space=pltpu.VMEM),
        scratch_shapes=[
            pltpu.VMEM((4, BS, BS), jnp.bfloat16),
            pltpu.SMEM((1, 1, 3), jnp.int32),
            pltpu.SMEM((64, 64), jnp.int32),
            pltpu.VMEM((48 * BS, BS), jnp.bfloat16),
            pltpu.VMEM((48 * BS, BS), jnp.bfloat16),
            pltpu.VMEM((48 * BS, BS), jnp.bfloat16),
            pltpu.VMEM((4, BS, LANES), jnp.bfloat16),
            pltpu.VMEM((2, 4, LANES, BS), jnp.bfloat16),
            pltpu.VMEM((2, BS, 3 * LANES), jnp.float32),
            pltpu.VMEM((3, BS, BS), jnp.float32),
            pltpu.SMEM((16, 9), jnp.int32),
            pltpu.SemaphoreType.DMA((3,)),
            pltpu.SemaphoreType.DMA((5,)),
            pltpu.SemaphoreType.DMA((NAMES,)),
        ],
        compiler_params=pltpu.CompilerParams(
            collective_id=0, has_side_effects=True, vmem_limit_bytes=67043328
        ),
        name="purify",
    )(tiles[0, 0], stack, mask)
    return result[None, None]


def solution(mesh):
    placed = (P("row", "col", None, None, None), P("row", "col", None), P())
    return jax.shard_map(
        local,
        mesh=mesh,
        in_specs=placed,
        out_specs=P("row", "col", None, None, None),
        check_vma=False,
    )
```
